128 devices in a mesh: row: 8 (over x, core), col: 4 (over z), layer: 4 (over y).
Axes of the slice: x: 4, y: 4, z: 4, core: 2. Of those that a mesh axis runs over, the one named last changes fastest.
Arguments:
- a_blocks: float32 [8, 128, 128, 128], P('row', ('col', 'layer')), may hold values from -0.5 to 0.5
- b_blocks: float32 [128, 4, 128, 128], P(('row', 'layer'), 'col'), may hold values from -2.5 to 2.5
- pair_plan: int32 [8, 4, 4, 8, 4, 3, 16], P('row', 'col', 'layer'), may hold values from 0 to 127, as said below
- pair_counts: int32 [8, 4, 4, 8, 4], P('row', 'col', 'layer'), may hold values from 0 to 16, as said below
Outputs:
- next_blocks: float32 [8, 4, 128, 128, 128], P('row', 'col', 'layer')
The draws below stay inside these ranges and needn't reach their ends.
Inputs may be any that keep to these rules, and one draw needn't show every extreme that they name: `pair_plan`: field 0 names a block of a_blocks whose index divided by 8 (rounded down) is congruent to m modulo 4; field 1 lies in 0 to 3 and field 2 in 0 to 31; entries past the count obey the same ranges. `pair_counts`: some entry equals 16 in every draw.
All inputs are finite; a program needn't handle non-finite values.
Results may differ from the reference program's by a relative error of at most 0.0003.
Values sent between devices are 32-bit elements; how exact they have to be, the bound alone decides.
A program may use at most 128 MiB of HBM per device.

```python
import jax
import jax.numpy as jnp
from jax import lax

BS = 128
ACAP = 8
BCAP = 4
PCAP = 16
CL = 32
N_ROW = 8
N_COL = 4
N_LAYER = 4


def draw_pair_plan(key, part):
    shape = (N_ROW, N_COL, N_LAYER, N_ROW, N_LAYER, PCAP)
    keys = jax.random.split(jax.random.fold_in(key, 11), 4)
    source_col = jax.random.randint(keys[0], shape, 0, N_COL)
    layer_ids = lax.broadcasted_iota(jnp.int32, shape, 4)
    within = jax.random.randint(keys[1], shape, 0, ACAP)
    left_ids = (source_col * N_LAYER + layer_ids) * ACAP + within
    right_ids = jax.random.randint(keys[2], shape, 0, BCAP)
    target = jax.random.randint(keys[3], shape, 0, CL)
    return jnp.stack([left_ids, right_ids, target], axis=5).astype(jnp.int32)


def draw_pair_counts(key, part):
    shape = (N_ROW, N_COL, N_LAYER, N_ROW, N_LAYER)
    keys = jax.random.split(jax.random.fold_in(key, 23), 3)
    level = jax.random.randint(keys[0], (N_ROW, N_COL, N_LAYER, 1, 1), 1, 5)
    upper = PCAP * level * level // 16
    lower = upper // 2
    spread = jax.random.randint(keys[1], shape, 0, PCAP + 1)
    counts = lower + spread % (upper - lower + 1)
    flat = counts.reshape(-1)
    chosen = jax.random.randint(keys[2], (), 0, flat.shape[0])
    flat = jnp.where(jnp.arange(flat.shape[0]) == chosen, PCAP, flat)
    return flat.reshape(shape).astype(jnp.int32)


def steps_of(rng, extent, cuts, low, largest):
    loudness = 1.0
    for position, parts in cuts:
        draws = jax.random.uniform(jax.random.fold_in(jax.random.fold_in(rng, 6), position), (parts,), jnp.float32, low / len(cuts), largest / len(cuts))
        loudness = loudness * jnp.repeat(jnp.exp(draws), extent[position] // parts).reshape((-1,) + (1,) * (len(extent) - 1 - position))
    return loudness


def gaussian(own_key, dims, scale, most, pieces=(), kind=jnp.bfloat16):
    drawn = jax.random.normal(own_key, dims, jnp.float32) * scale
    if len(pieces) > 0:
        drawn = steps_of(own_key, dims, pieces, -0.22, 0.18) * drawn
    return jnp.clip(drawn, min=-most, max=most).astype(kind)


def setup_inputs(seed: int = 0) -> dict:
    streams_of = jax.random.split(jax.random.key(seed), 5)
    return {
        "a_blocks": gaussian(streams_of[0], (N_ROW, N_COL * N_LAYER * ACAP, BS, BS), BS ** -0.5, 0.5, ((0, 8), (1, 16)), jnp.float32),
        "b_blocks": gaussian(streams_of[1], (N_ROW * N_LAYER * BCAP, N_COL, BS, BS), ((3 * CL / (N_ROW * N_LAYER * PCAP)) ** 0.5), 2.5, ((0, 32), (1, 4)), jnp.float32),
        "pair_plan": draw_pair_plan(jax.random.fold_in(streams_of[4], 71), 0),
        "pair_counts": draw_pair_counts(jax.random.fold_in(streams_of[4], 71), 0),
    }


def reference(a_blocks, b_blocks, pair_plan, pair_counts):
    devices = N_ROW * N_COL * N_LAYER
    sources = N_ROW * N_LAYER
    plans = pair_plan.reshape(devices, sources, 3, PCAP)
    counts = pair_counts.reshape(devices, sources)
    device_ids = jnp.arange(devices, dtype=jnp.int32)

    def one_device(item):
        ident, plan, count = item
        row_id = (ident // (N_COL * N_LAYER)).astype(jnp.int32)
        col_id = ((ident // N_LAYER) % N_COL).astype(jnp.int32)
        left_blocks = lax.dynamic_index_in_dim(a_blocks, row_id, 0, keepdims=False)
        right_blocks = lax.dynamic_index_in_dim(b_blocks, col_id, 1, keepdims=False)
        source_ids = jnp.arange(sources, dtype=jnp.int32)[:, None]
        left_ids = plan[:, 0, :].reshape(-1)
        right_ids = (plan[:, 1, :] + source_ids * BCAP).reshape(-1)
        target = plan[:, 2, :].reshape(-1)
        live = (jnp.arange(PCAP, dtype=jnp.int32)[None, :] < count[:, None]).reshape(-1)
        lhs = jnp.take(left_blocks, left_ids, axis=0)
        rhs = jnp.take(right_blocks, right_ids, axis=0)
        products = jnp.einsum("pij,pjk->pik", lhs, rhs, precision=lax.Precision.HIGHEST)
        products = jnp.where(live[:, None, None], products, jnp.zeros_like(products))
        return jax.ops.segment_sum(products, target, num_segments=CL)

    result = lax.map(one_device, (device_ids, plans, counts))
    return result.reshape(N_ROW, N_COL, N_LAYER * CL, BS, BS)
```

```python
import jax
import jax.numpy as jnp
from jax import lax
from jax.experimental import pallas as pl
from jax.experimental.pallas import tpu as pltpu
from jax.sharding import PartitionSpec as P

BS = 128
ACAP = 8
BCAP = 4
PCAP = 16
CL = 32
N_ROW, N_COL, N_LAYER = 8, 4, 4
N_X = N_ROW // 2
A_ROWS = ACAP * BS
B_ROWS = BCAP * BS
Y_FIRST = 592
LISTS = N_ROW
PHASE = LISTS * PCAP
GROUP = 2
MESH = pl.DeviceIdType.MESH


def messages():
    out = {}

    def ring(tag, plus, minus, slot, rows, needs):
        start, stop = rows
        middle = (start + stop) // 2
        own = slot(0)
        up, down = tag + "+", tag + "-"
        out[up] = (plus, own, slot(3), rows, needs)
        out[down] = (minus, own, slot(1), rows, needs)
        out[up + "2"] = (plus, slot(3), slot(2), (start, middle), [up])
        out[down + "2"] = (minus, slot(1), slot(2), (middle, stop), [down])
        return {0: needs, 3: [up], 1: [down], 2: [up + "2", down + "2"]}

    first, second, whole = (0, Y_FIRST), (Y_FIRST, A_ROWS), (0, B_ROWS)
    by_layer = ring("By", "Y+", "Y-", lambda d: ("B", d, 0, 0), whole, [])
    a_layer = ring("Fy", "Y+", "Y-", lambda d: ("A", d, 0), first, [])
    a_col = ring("Gz", "Z+", "Z-", lambda e: ("A", 0, e), second, [])
    for d in (0, 3, 1, 2):
        ring(f"Bx{d}", "X+", "X-", lambda x: ("B", d, x, 0), whole, by_layer[d])
        ring(f"Fz{d}", "Z+", "Z-", lambda e: ("A", d, e), first, a_layer[d])
        ring(f"Gy{d}", "Y+", "Y-", lambda q: ("A", q, d), second, a_col[d])
    out["D"] = ("D", ("B", 0, 0, 0), ("B", 0, 0, 1), whole, [])
    for name in [n for n in out if n[0] == "B"]:
        _, _, target, rows, _ = out[name]
        out["D" + name] = ("D", target, target[:3] + (1,), rows, [name])
    return out


FIRST_SENDS = (
    "Gz+", "Gz-", "Fy+", "Fy-", "By+", "By-", "Bx0+", "Bx0-",
    "Fz0+", "Fz0-", "D", "Gy0+", "Gy0-",
)


def schedule():
    table = messages()
    row_time = {"D": 1.0}
    latency = {"D": 1100.0}
    ready_at, free_at, waited, started, steps = {}, {}, set(), set(), []
    now = 0.0

    def send(name):
        queue, _, _, (start, stop), _ = table[name]
        begin = max(now, free_at.get(queue, 0.0))
        free_at[queue] = begin + (stop - start) * row_time.get(queue, 11.0)
        ready_at[name] = free_at[queue] + latency.get(queue, 2000.0)
        started.add(name)
        steps.append(("send", name))

    for name in FIRST_SENDS:
        send(name)
    arrived_rows = {("A", 0, 0): A_ROWS, ("B", 0, 0, 0): B_ROWS}
    split, phases = set(), [(d, g) for d in (0, 3, 1, 2) for g in range(LISTS // GROUP)]
    slots = [("A", d, e) for d in range(4) for e in range(4)]
    slots += [("B", d, x, k) for d in range(4) for x in range(4) for k in range(2)]

    def task():
        if phases:
            d, g = phases[0]
            if all(s in split for s in slots if s[1] == d):
                phases.pop(0)
                return ("multiply", d, g), 420.0 * GROUP
        for s in sorted(slots, key=lambda s: ((0, 3, 1, 2).index(s[1]), s)):
            if s not in split and arrived_rows.get(s, 0) == (A_ROWS if s[0] == "A" else B_ROWS):
                split.add(s)
                return ("split", s), 300.0 if s[0] == "A" else 150.0
        return None

    while len(waited) < len(table) or phases:
        pending = sorted((ready_at[n], n) for n in started if n not in waited)
        if pending and pending[0][0] <= now:
            name = pending[0][1]
            waited.add(name)
            steps.append(("wait", name))
            target, (start, stop) = table[name][2], table[name][3]
            arrived_rows[target] = arrived_rows.get(target, 0) + stop - start
            for other, entry in table.items():
                if other not in started and all(n in waited for n in entry[4]):
                    send(other)
            continue
        chosen = task()
        if chosen is not None:
            steps.append(chosen[0])
            now += chosen[1]
        else:
            now = pending[0][0]
    return table, steps, now, free_at


def kernel(plan, a_ref, b_ref, out_ref, a_land, b_land, a_half, b_half, chain, send_sem, recv_sem):
    r, c, o = lax.axis_index("row"), lax.axis_index("col"), lax.axis_index("layer")
    devices = {
        "X+": (lax.rem(r + 2, N_ROW), c, o),
        "X-": (lax.rem(r + N_ROW - 2, N_ROW), c, o),
        "D": (r + 1 - 2 * lax.rem(r, 2), c, o),
        "Y+": (r, c, lax.rem(o + 1, N_LAYER)),
        "Y-": (r, c, lax.rem(o + N_LAYER - 1, N_LAYER)),
        "Z+": (r, lax.rem(c + 1, N_COL), o),
        "Z-": (r, lax.rem(c + N_COL - 1, N_COL), o),
    }
    table, steps, _, _ = schedule()

    def view(slot, rows):
        window = pl.ds(rows[0], rows[1] - rows[0])
        if slot == ("A", 0, 0):
            return a_ref.at[window]
        if slot == ("B", 0, 0, 0):
            return b_ref.at[window]
        if slot[0] == "A":
            return a_land.at[slot[1], slot[2], window]
        return b_land.at[slot[1], slot[2], slot[3], window]

    copies = {}
    for number, (name, (queue, source, target, rows, _)) in enumerate(table.items()):
        copies[name] = pltpu.make_async_remote_copy(
            src_ref=view(source, rows),
            dst_ref=view(target, rows),
            send_sem=send_sem.at[number],
            recv_sem=recv_sem.at[number],
            device_id=devices[queue],
            device_id_type=MESH,
        )

    barrier = pltpu.get_barrier_semaphore()
    for device in devices.values():
        pl.semaphore_signal(barrier, inc=1, device_id=device, device_id_type=MESH)
    pl.semaphore_wait(barrier, len(devices))

    def split(slot):
        if slot[0] == "A":
            base, blocks, halves = slot[2] * ACAP, ACAP, a_half
        else:
            base, blocks, halves = (slot[2] * 2 + slot[3]) * BCAP, BCAP, b_half
        source = view(slot, (0, blocks * BS))

        def one(block, carry):
            value = source[pl.ds(pl.multiple_of(block * BS, BS), BS), :]
            high = value.astype(jnp.bfloat16)
            low = (value - high.astype(jnp.float32)).astype(jnp.bfloat16)
            halves[slot[1], base + block, :, 0:BS] = high
            halves[slot[1], base + block, :, BS : 2 * BS] = low
            return carry

        lax.fori_loop(0, blocks, one, 0)

    def multiply(d, group):
        def one_list(index, carry):
            for p in range(PCAP):
                at = index * PCAP + p
                left = a_half[d, plan[d * PHASE + at]]
                right = b_half[d, plan[(4 + d) * PHASE + at]]
                both = jnp.dot(
                    left,
                    jnp.concatenate([right, right], axis=0),
                    preferred_element_type=jnp.float32,
                )
                before = chain[plan[(8 + d) * PHASE + at]]
                chain[at] = before + (both[:, 0:BS] + both[:, BS : 2 * BS])
            return carry

        lax.fori_loop(group * GROUP, (group + 1) * GROUP, one_list, 0)

    def collect(d, last):
        def one(t, carry):
            total = chain[plan[12 * PHASE + d * CL + t]]
            if last:
                out_ref[t] = total
            else:
                chain[PHASE + t] = total
            return carry

        lax.fori_loop(0, CL, one, 0)

    def clear(t, carry):
        chain[t] = jnp.zeros((BS, BS), jnp.float32)
        return carry

    cleared = False
    for step in steps:
        if step[0] == "send":
            copies[step[1]].start()
            continue
        if not cleared:
            lax.fori_loop(0, PHASE + CL, clear, 0)
            cleared = True
        if step[0] == "wait":
            copies[step[1]].wait_recv()
        elif step[0] == "split":
            split(step[1])
        else:
            _, d, group = step
            multiply(d, group)
            if group == LISTS // GROUP - 1:
                collect(d, d == 2)
    for copy in copies.values():
        copy.wait_send()


def tables(pair_plan, pair_counts):
    r, c, o = lax.axis_index("row"), lax.axis_index("col"), lax.axis_index("layer")
    phase = lax.rem(o + jnp.arange(N_LAYER, dtype=jnp.int32), N_LAYER)
    plan = jnp.take(pair_plan, phase, axis=1)
    counts = jnp.take(pair_counts, phase, axis=1)
    plan = jnp.moveaxis(plan, 0, 1)
    counts = jnp.moveaxis(counts, 0, 1)
    left, right, target = plan[:, :, 0], plan[:, :, 1], plan[:, :, 2]
    column = lax.rem(left // (N_LAYER * ACAP) + N_COL - c, N_COL)
    a_at = column * ACAP + left % ACAP
    s = jnp.arange(N_ROW, dtype=jnp.int32)
    x_on = lax.rem(s // 2 + N_X - r // 2, N_X)
    core_on = lax.rem(s + r, 2)
    b_at = ((x_on * 2 + core_on) * BCAP)[None, :, None] + right
    live = jnp.arange(PCAP, dtype=jnp.int32) < counts[:, :, None]
    key = jnp.where(live, target, -1).reshape(N_LAYER, PHASE)
    target = target.reshape(N_LAYER, PHASE)
    at = jnp.arange(PHASE, dtype=jnp.int32)
    earlier = (key[:, None, :] == target[:, :, None]) & (at[None, :] < at[:, None])
    previous = jnp.max(jnp.where(earlier, at, -1), axis=2)
    previous = jnp.where(previous < 0, PHASE + target, previous)
    result = jnp.arange(CL, dtype=jnp.int32)
    named = key[:, None, :] == result[:, None]
    last = jnp.max(jnp.where(named, at, -1), axis=2)
    last = jnp.where(last < 0, PHASE + result, last)
    parts = [a_at.reshape(-1), b_at.reshape(-1), previous.reshape(-1), last.reshape(-1)]
    return jnp.concatenate(parts)


def per_device(a_blocks, b_blocks, pair_plan, pair_counts):
    plan = tables(pair_plan[0, 0, 0], pair_counts[0, 0, 0])
    count = len(messages())
    vmem = pl.BlockSpec(memory_space=pltpu.VMEM)
    result = pl.pallas_call(
        kernel,
        out_shape=jax.ShapeDtypeStruct((CL, BS, BS), jnp.float32),
        in_specs=[pl.BlockSpec(memory_space=pltpu.SMEM), vmem, vmem],
        out_specs=vmem,
        scratch_shapes=[
            pltpu.VMEM((N_LAYER, N_COL, A_ROWS, BS), jnp.float32),
            pltpu.VMEM((N_LAYER, N_X, 2, B_ROWS, BS), jnp.float32),
            pltpu.VMEM((N_LAYER, N_COL * ACAP, BS, 2 * BS), jnp.bfloat16),
            pltpu.VMEM((N_LAYER, N_ROW * BCAP, BS, 2 * BS), jnp.bfloat16),
            pltpu.VMEM((PHASE + CL, BS, BS), jnp.float32),
            pltpu.SemaphoreType.DMA((count,)),
            pltpu.SemaphoreType.DMA((count,)),
        ],
        compiler_params=pltpu.CompilerParams(
            collective_id=0, has_side_effects=True, vmem_limit_bytes=60 * 1024 * 1024
        ),
        name="gather_multiply",
    )(plan, a_blocks.reshape(A_ROWS, BS), b_blocks.reshape(B_ROWS, BS))
    return result[None, None]


def solution(mesh):
    in_specs = (
        P("row", ("col", "layer"), None, None),
        P(("row", "layer"), "col", None, None),
        P("row", "col", "layer", None, None, None, None),
        P("row", "col", "layer", None, None),
    )
    out_specs = P("row", "col", "layer", None, None)
    return jax.shard_map(
        per_device, mesh=mesh, in_specs=in_specs, out_specs=out_specs, check_vma=False
    )
```

```python
import jax
import jax.numpy as jnp
from jax import lax
from jax.experimental import pallas as pl
from jax.experimental.pallas import tpu as pltpu
from jax.sharding import PartitionSpec as P

BS = 128
ACAP = 8
BCAP = 4
PCAP = 16
CL = 32
N_ROW, N_COL, N_LAYER = 8, 4, 4
N_X = N_ROW // 2
LISTS = N_ROW
PHASE = LISTS * PCAP
GROUPS = 2
UNROLL = 64
ORDER = (0, 3, 1, 2)
MESH = pl.DeviceIdType.MESH


def messages():
    out = {}

    def put(name, *entry):
        out[name] = entry

    put("Fy+", "Y+", ("A", 0, 0), ("A", 3, 0), (0, 6), [])
    put("Fy-", "Y-", ("A", 0, 0), ("A", 1, 0), (4, 8), [])
    put("Hy+", "Y+", ("A", 0, 0), ("A", 3, 0), (6, 8), [])
    put("Hy-", "Y-", ("A", 0, 0), ("A", 1, 0), (0, 4), [])
    put("Fy+2", "Y+", ("A", 3, 0), ("A", 2, 0), (0, 4), ["Fy+"])
    put("Fy-2", "Y-", ("A", 1, 0), ("A", 2, 0), (4, 8), ["Fy-"])
    put("Gz+", "Z+", ("A", 0, 0), ("A", 0, 3), (0, 4), [])
    put("Gz-", "Z-", ("A", 0, 0), ("A", 0, 1), (4, 8), [])
    put("Iz+", "Z+", ("A", 0, 0), ("A", 0, 3), (4, 8), [])
    put("Iz-", "Z-", ("A", 0, 0), ("A", 0, 1), (0, 4), [])
    put("Gz+2", "Z+", ("A", 0, 3), ("A", 0, 2), (0, 4), ["Gz+"])
    put("Gz-2", "Z-", ("A", 0, 1), ("A", 0, 2), (4, 8), ["Gz-"])
    put("Fz3+", "Z+", ("A", 3, 0), ("A", 3, 3), (0, 3), ["Fy+"])
    put("Fz3-", "Z-", ("A", 3, 0), ("A", 3, 1), (3, 6), ["Fy+"])
    put("Iz3+", "Z+", ("A", 3, 0), ("A", 3, 3), (3, 6), ["Fy+"])
    put("Iz3-", "Z-", ("A", 3, 0), ("A", 3, 1), (0, 3), ["Fy+"])
    put("Fz3+2", "Z+", ("A", 3, 3), ("A", 3, 2), (0, 3), ["Fz3+"])
    put("Fz3-2", "Z-", ("A", 3, 1), ("A", 3, 2), (3, 6), ["Fz3-"])
    put("Fz1+", "Z+", ("A", 1, 0), ("A", 1, 3), (4, 6), ["Fy-"])
    put("Fz1-", "Z-", ("A", 1, 0), ("A", 1, 1), (6, 8), ["Fy-"])
    put("Iz1+", "Z+", ("A", 1, 0), ("A", 1, 3), (6, 8), ["Fy-"])
    put("Iz1-", "Z-", ("A", 1, 0), ("A", 1, 1), (4, 6), ["Fy-"])
    put("Fz1+2", "Z+", ("A", 1, 3), ("A", 1, 2), (4, 6), ["Fz1+"])
    put("Fz1-2", "Z-", ("A", 1, 1), ("A", 1, 2), (6, 8), ["Fz1-"])
    upper = {3: ["Iz+"], 1: ["Gz-"], 2: ["Gz-2"]}
    lower = {3: ["Gz+"], 1: ["Iz-"], 2: ["Gz+2"]}
    for e in (3, 1, 2):
        put(f"Gy{e}+", "Y+", ("A", 0, e), ("A", 3, e), (6, 8), upper[e])
        put(f"Gy{e}-", "Y-", ("A", 0, e), ("A", 1, e), (0, 4), lower[e])
    fifth = {3: ["Iz3+"], 1: ["Fz3-"], 2: ["Fz3-2"]}
    fourth = {3: ["Fz1+"], 1: ["Iz1-"], 2: ["Fz1+2"]}
    for e in (3, 1, 2):
        put(f"Gy{e}+2", "Y+", ("A", 3, e), ("A", 2, e), (5, 8), [f"Gy{e}+"] + fifth[e])
        put(f"Gy{e}-2", "Y-", ("A", 1, e), ("A", 2, e), (4, 5), fourth[e])
    put("Fz2+", "Z+", ("A", 2, 0), ("A", 2, 3), (0, 2), ["Fy+2"])
    put("Fz2-", "Z-", ("A", 2, 0), ("A", 2, 1), (2, 4), ["Fy+2"])
    put("Iz2+", "Z+", ("A", 2, 0), ("A", 2, 3), (2, 4), ["Fy+2"])
    put("Iz2-", "Z-", ("A", 2, 0), ("A", 2, 1), (0, 2), ["Fy+2"])
    put("Fz2+2", "Z+", ("A", 2, 3), ("A", 2, 2), (0, 2), ["Fz2+"])
    put("Fz2-2", "Z-", ("A", 2, 1), ("A", 2, 2), (2, 4), ["Fz2-"])
    put("By+", "Y+", ("B", 0, 0, 0), ("B", 3, 0, 0), (0, 4), [])
    put("By-", "Y-", ("B", 0, 0, 0), ("B", 1, 0, 0), (0, 4), [])
    put("By+2", "Y+", ("B", 3, 0, 0), ("B", 2, 0, 0), (0, 2), ["By+"])
    put("By-2", "Y-", ("B", 1, 0, 0), ("B", 2, 0, 0), (2, 4), ["By-"])
    layer = {0: [], 3: ["By+"], 1: ["By-"], 2: ["By+2", "By-2"]}
    for d in ORDER:
        put(f"Bx{d}+", "X+", ("B", d, 0, 0), ("B", d, 3, 0), (0, 4), layer[d])
        put(f"Bx{d}-", "X-", ("B", d, 0, 0), ("B", d, 1, 0), (0, 4), layer[d])
        put(f"Bx{d}+2", "X+", ("B", d, 3, 0), ("B", d, 2, 0), (0, 2), [f"Bx{d}+"])
        put(f"Bx{d}-2", "X-", ("B", d, 1, 0), ("B", d, 2, 0), (2, 4), [f"Bx{d}-"])
        sources = {0: layer[d], 3: [f"Bx{d}+"], 1: [f"Bx{d}-"], 2: [f"Bx{d}+2", f"Bx{d}-2"]}
        for x, needs in sources.items():
            put(f"D{d}{x}", "D", ("B", d, x, 0), ("B", d, x, 1), (0, 4), needs)
    return out


Z_ORDER = (
    "Gz*", "Iz*", "Gz*2", "Fz3*", "Iz3*", "Fz3*2", "Fz1*", "Iz1*", "Fz1*2", "Fz2*", "Iz2*", "Fz2*2",
)
Y_ORDER = (
    "By*", "Fy*", "Hy*", "By*2", "Gy3*", "Gy1*", "Gy2*", "Fy*2", "Gy3*2", "Gy1*2", "Gy2*2",
)
X_ORDER = ("Bx0*", "Bx0*2", "Bx3*", "Bx1*", "Bx3*2", "Bx1*2", "Bx2*", "Bx2*2")


AFTER = {0: ("Gz+2", "Gz-2"), 3: ("Fz1+", "Fz1-"), 1: ("Fz2+", "Fz2-"), 2: ()}


def groups():
    out = {"By2": ("By+2", "By-2"), "Gy+": ("Gy3+", "Gy1+", "Gy2+"), "Gy-": ("Gy3-", "Gy1-", "Gy2-")}
    for d in ORDER:
        out[f"Bx{d}2"] = (f"Bx{d}+2", f"Bx{d}-2")
        out[f"D{d}"] = tuple(f"D{d}{x}" for x in range(N_X))
    grouped = {n for names in out.values() for n in names}
    out.update({n: (n,) for n in messages() if n not in grouped})
    return out


def schedule():
    table = messages()
    ready_at, free_at, waited, started, steps = {}, {}, set(), set(), []
    now = 0.0

    def send(name):
        queue, _, _, blocks, _ = table[name]
        begin = max(now, free_at.get(queue, 0.0))
        free_at[queue] = begin + (blocks[1] - blocks[0]) * (128.0 if queue == "D" else 1420.0)
        ready_at[name] = free_at[queue] + (1100.0 if queue == "D" else 2400.0)
        started.add(name)
        steps.append(("send", name))

    order = {
        axis + sign: [n.replace("*", sign) for n in names]
        for axis, names in (("Z", Z_ORDER), ("Y", Y_ORDER), ("X", X_ORDER))
        for sign in "+-"
    }

    def send_ready():
        for names in order.values():
            while names and all(n in waited for n in table[names[0]][4]):
                send(names.pop(0))
        for name, entry in table.items():
            if entry[0] == "D" and name not in started and all(n in waited for n in entry[4]):
                send(name)

    send_ready()
    steps.append(("tables",))
    now += 2500.0
    ripe = [(("A", 0, 0), (0, ACAP)), (("B", 0, 0, 0), (0, BCAP))]
    missing = {d: N_COL * ACAP + N_ROW * BCAP for d in ORDER}
    phases = [(d, g) for d in ORDER for g in range(GROUPS)]
    together = groups()

    def task():
        if phases and missing[phases[0][0]] == 0 and all(n in waited for n in AFTER[phases[0][0]]):
            d, g = phases.pop(0)
            return ("multiply", d, g), 2500.0 / GROUPS + (400.0 if g == GROUPS - 1 else 0.0)
        if ripe:
            slot, blocks = ripe.pop(min(range(len(ripe)), key=lambda i: ORDER.index(ripe[i][0][1])))
            missing[slot[1]] -= blocks[1] - blocks[0]
            return ("split", slot, blocks), 35.0 * (blocks[1] - blocks[0]) + 30.0
        return None

    while len(waited) < len(table) or phases:
        pending = sorted(
            (max(ready_at[n] for n in names), group)
            for group, names in together.items()
            if all(n in started for n in names) and names[0] not in waited
        )
        if pending and pending[0][0] <= now:
            group = pending[0][1]
            waited.update(together[group])
            steps.append(("wait", group))
            ripe.extend(table[n][2:4] for n in together[group])
            send_ready()
            continue
        chosen = task()
        if chosen is not None:
            steps.append(chosen[0])
            now += chosen[1]
        else:
            now = pending[0][0]
    return table, steps, now, free_at


def kernel(
    a_ref, b_ref, plan_ref, counts_ref, out_ref,
    a_land, b_land, a_half, b_half, chain, sums, plan_v, counts_v, table_v, table_s, own_sem, send_sem, recv_sem,
):
    r, c, o = lax.axis_index("row"), lax.axis_index("col"), lax.axis_index("layer")
    devices = {
        "X+": (lax.rem(r + 2, N_ROW), c, o),
        "X-": (lax.rem(r + N_ROW - 2, N_ROW), c, o),
        "D": (r + 1 - 2 * lax.rem(r, 2), c, o),
        "Y+": (r, c, lax.rem(o + 1, N_LAYER)),
        "Y-": (r, c, lax.rem(o + N_LAYER - 1, N_LAYER)),
        "Z+": (r, lax.rem(c + 1, N_COL), o),
        "Z-": (r, lax.rem(c + N_COL - 1, N_COL), o),
    }
    own = [
        pltpu.make_async_copy(a_ref, a_land.at[0, 0], own_sem.at[0]),
        pltpu.make_async_copy(b_ref, b_land.at[0, 0, 0], own_sem.at[1]),
        pltpu.make_async_copy(plan_ref, plan_v, own_sem.at[2]),
        pltpu.make_async_copy(counts_ref, counts_v, own_sem.at[3]),
    ]
    to_scalar = pltpu.make_async_copy(table_v, table_s, own_sem.at[4])
    for copy in own:
        copy.start()
    barrier = pltpu.get_barrier_semaphore()
    for device in devices.values():
        pl.semaphore_signal(barrier, inc=1, device_id=device, device_id_type=MESH)
    pl.semaphore_wait(barrier, len(devices))
    own[0].wait()
    own[1].wait()

    table, steps, _, _ = schedule()

    def view(slot, blocks):
        land = a_land if slot[0] == "A" else b_land
        return land.at[(*slot[1:], pl.ds(blocks[0], blocks[1] - blocks[0]))]

    together = groups()
    number = {n: i for i, names in enumerate(together.values()) for n in names}
    copies, sent, size = {}, [0, 0], [0] * len(together)
    for name, (queue, source, target, blocks, _) in table.items():
        pool = 0 if queue[0] in "YZ" else 1
        sent[pool] += blocks[1] - blocks[0]
        size[number[name]] += blocks[1] - blocks[0]
        copies[name] = pltpu.make_async_remote_copy(
            src_ref=view(source, blocks),
            dst_ref=view(target, blocks),
            send_sem=send_sem.at[pool],
            recv_sem=recv_sem.at[number[name]],
            device_id=devices[queue],
            device_id_type=MESH,
        )

    def make_tables():
        own[2].wait()
        own[3].wait()
        shape = (N_LAYER, PHASE)
        fields = [
            jnp.concatenate([plan_v[s, f] for s in range(LISTS)], axis=1) for f in range(3)
        ]
        limit = jnp.concatenate(
            [jnp.broadcast_to(counts_v[:, s : s + 1], (N_LAYER, PCAP)) for s in range(LISTS)], axis=1
        )
        left, right, target = fields
        at = lax.broadcasted_iota(jnp.int32, shape, 1)
        s = at // PCAP
        column = (left // (N_LAYER * ACAP) + N_COL - c) % N_COL
        x_on = (s // 2 + N_X - r // 2) % N_X
        core_on = (s + r) % 2
        live = at % PCAP < limit
        key = jnp.where(live, target, CL) * PHASE + at
        packed = (target * PHASE + column * ACAP + left % ACAP) * PHASE
        packed = packed + (x_on * 2 + core_on) * BCAP + right
        rank = jnp.zeros(shape, jnp.int32)
        for q in range(PHASE):
            rank += jnp.where(jnp.broadcast_to(key[:, q : q + 1], shape) < key, 1, 0)
        ordered, place, last = packed, target, jnp.full(shape, -1, jnp.int32)
        sort_key = key // PHASE
        for q in range(PHASE):
            here = at == jnp.broadcast_to(rank[:, q : q + 1], shape)
            ordered = jnp.where(here, jnp.broadcast_to(packed[:, q : q + 1], shape), ordered)
            place = jnp.where(here, jnp.broadcast_to(sort_key[:, q : q + 1], shape), place)
            one = jnp.broadcast_to(sort_key[:, q : q + 1], shape)
            last = jnp.where(at == one, jnp.maximum(last, jnp.broadcast_to(rank[:, q : q + 1], shape)), last)
        earlier = jnp.concatenate([place[:, 0:1] - 1, place[:, 0 : PHASE - 1]], axis=1)
        table_v[0:4] = ordered // PHASE % PHASE
        table_v[4:8] = ordered % PHASE
        table_v[8:12] = ordered // (PHASE * PHASE)
        table_v[12:16] = jnp.where(place == earlier, 0, 1)
        table_v[16:20] = jnp.where(last < 0, PHASE + at, last)

    def wait_for(sem, blocks):
        window = chain.at[pl.ds(0, blocks)]
        pltpu.make_async_copy(window, window, sem).wait()

    def split(slot, blocks):
        if slot[0] == "A":
            base, halves, land = slot[2] * ACAP, a_half, a_land
        else:
            base, halves, land = (slot[2] * 2 + slot[3]) * BCAP, b_half, b_land

        def one(block, carry):
            value = land[(*slot[1:], block)]
            high = value.astype(jnp.bfloat16)
            low = (value - high.astype(jnp.float32)).astype(jnp.bfloat16)
            halves[slot[1], base + block, :, 0:BS] = high
            halves[slot[1], base + block, :, BS : 2 * BS] = low
            return carry

        lax.fori_loop(*blocks, one, 0)

    def multiply(d, total, group):
        m = lax.rem(o + d, N_LAYER)
        steps_of_group = PHASE // GROUPS // UNROLL

        def some(index, total):
            for p in range(UNROLL):
                at = index * UNROLL + p
                left = a_half[d, table_s[m, at]]
                right = b_half[d, table_s[4 + m, at]]
                both = jnp.dot(
                    left,
                    jnp.concatenate([right, right], axis=0),
                    preferred_element_type=jnp.float32,
                )
                first = jnp.broadcast_to(table_s[12 + m, at], (BS, BS)) == 1
                total = jnp.where(first, sums[table_s[8 + m, at]], total)
                total = total + (both[:, 0:BS] + both[:, BS : 2 * BS])
                chain[at] = total
            return total

        return lax.fori_loop(group * steps_of_group, (group + 1) * steps_of_group, some, total)

    def collect(d):
        m = lax.rem(o + d, N_LAYER)

        def one(t, carry):
            at = table_s[16 + m, t]
            total = jnp.where(
                jnp.broadcast_to(at, (BS, BS)) < PHASE, chain[jnp.minimum(at, PHASE - 1)], sums[t]
            )
            if d == ORDER[-1]:
                out_ref[t] = total
            else:
                sums[t] = total
            return carry

        lax.fori_loop(0, CL, one, 0)

    def clear(t, carry):
        sums[t] = jnp.zeros((BS, BS), jnp.float32)
        return carry

    scalars, running = "none", jnp.zeros((BS, BS), jnp.float32)
    for step in steps:
        if step[0] == "send":
            copies[step[1]].start()
        elif step[0] == "tables":
            make_tables()
            lax.fori_loop(0, CL, clear, 0)
        elif step[0] == "wait":
            names = together[step[1]]
            if len(names) == 1:
                copies[names[0]].wait_recv()
            else:
                wait_for(recv_sem.at[number[names[0]]], size[number[names[0]]])
            if scalars == "none":
                to_scalar.start()
                scalars = "started"
        elif step[0] == "split":
            split(*step[1:])
        else:
            if scalars == "started":
                to_scalar.wait()
                scalars = "there"
            running = multiply(step[1], running, step[2])
            if step[2] == GROUPS - 1:
                collect(step[1])
    for pool in range(2):
        wait_for(send_sem.at[pool], sent[pool])


def per_device(a_blocks, b_blocks, pair_plan, pair_counts):
    count = len(groups())
    hbm = pl.BlockSpec(memory_space=pltpu.HBM)
    plan = pair_plan[0, 0, 0].transpose(0, 2, 1, 3)
    operands = (a_blocks[0], b_blocks[:, 0], plan, pair_counts[0, 0, 0].T)
    result = pl.pallas_call(
        kernel,
        out_shape=jax.ShapeDtypeStruct((CL, BS, BS), jnp.float32),
        in_specs=[hbm, hbm, hbm, hbm],
        out_specs=pl.BlockSpec(memory_space=pltpu.VMEM),
        scratch_shapes=[
            pltpu.VMEM((N_LAYER, N_COL, ACAP, BS, BS), jnp.float32),
            pltpu.VMEM((N_LAYER, N_X, 2, BCAP, BS, BS), jnp.float32),
            pltpu.VMEM((N_LAYER, N_COL * ACAP, BS, 2 * BS), jnp.bfloat16),
            pltpu.VMEM((N_LAYER, N_ROW * BCAP, BS, 2 * BS), jnp.bfloat16),
            pltpu.VMEM((PHASE + BCAP, BS, BS), jnp.float32),
            pltpu.VMEM((CL, BS, BS), jnp.float32),
            pltpu.VMEM((N_ROW, 3, N_LAYER, PCAP), jnp.int32),
            pltpu.VMEM((N_LAYER, N_ROW), jnp.int32),
            pltpu.VMEM((24, PHASE), jnp.int32),
            pltpu.SMEM((24, PHASE), jnp.int32),
            pltpu.SemaphoreType.DMA((5,)),
            pltpu.SemaphoreType.DMA((2,)),
            pltpu.SemaphoreType.DMA((count,)),
        ],
        compiler_params=pltpu.CompilerParams(
            collective_id=0, has_side_effects=True, vmem_limit_bytes=50 * 1024 * 1024
        ),
        name="gather_multiply",
    )(*[pltpu.with_memory_space_constraint(x, pltpu.HBM) for x in operands])
    return result[None, None]


def solution(mesh):
    in_specs = (
        P("row", ("col", "layer"), None, None),
        P(("row", "layer"), "col", None, None),
        P("row", "col", "layer", None, None, None, None),
        P("row", "col", "layer", None, None),
    )
    out_specs = P("row", "col", "layer", None, None)
    return jax.shard_map(
        per_device, mesh=mesh, in_specs=in_specs, out_specs=out_specs, check_vma=False
    )
```

```python
import jax
import jax.numpy as jnp
from jax import lax
from jax.experimental import pallas as pl
from jax.experimental.pallas import tpu as pltpu
from jax.sharding import PartitionSpec as P

BS = 128
ACAP = 8
BCAP = 4
PCAP = 16
CL = 32
N_ROW, N_COL, N_LAYER = 8, 4, 4
N_X = N_ROW // 2
LISTS = N_ROW
PHASE = LISTS * PCAP
UNROLL = {0: 32, 3: 32, 1: 32, 2: 128}
ORDER = (0, 3, 1, 2)
MESH = pl.DeviceIdType.MESH


def messages():
    out = {}

    def put(name, *entry):
        out[name] = entry

    put("Fy+", "Y+", ("A", 0, 0), ("A", 3, 0), (0, 6), [])
    put("Fy-", "Y-", ("A", 0, 0), ("A", 1, 0), (4, 8), [])
    put("Hy+", "Y+", ("A", 0, 0), ("A", 3, 0), (6, 8), [])
    put("Hy-", "Y-", ("A", 0, 0), ("A", 1, 0), (0, 4), [])
    put("Fy+2", "Y+", ("A", 3, 0), ("A", 2, 0), (0, 4), ["Fy+"])
    put("Fy-2", "Y-", ("A", 1, 0), ("A", 2, 0), (4, 8), ["Fy-"])
    put("Gz+", "Z+", ("A", 0, 0), ("A", 0, 3), (0, 4), [])
    put("Gz-", "Z-", ("A", 0, 0), ("A", 0, 1), (4, 8), [])
    put("Iz+", "Z+", ("A", 0, 0), ("A", 0, 3), (4, 8), [])
    put("Iz-", "Z-", ("A", 0, 0), ("A", 0, 1), (0, 4), [])
    put("Gz+2", "Z+", ("A", 0, 3), ("A", 0, 2), (0, 4), ["Gz+"])
    put("Gz-2", "Z-", ("A", 0, 1), ("A", 0, 2), (4, 8), ["Gz-"])
    put("Fz3+", "Z+", ("A", 3, 0), ("A", 3, 3), (0, 3), ["Fy+"])
    put("Fz3-", "Z-", ("A", 3, 0), ("A", 3, 1), (3, 6), ["Fy+"])
    put("Iz3+", "Z+", ("A", 3, 0), ("A", 3, 3), (3, 6), ["Fy+"])
    put("Iz3-", "Z-", ("A", 3, 0), ("A", 3, 1), (0, 3), ["Fy+"])
    put("Fz3+2", "Z+", ("A", 3, 3), ("A", 3, 2), (0, 3), ["Fz3+"])
    put("Fz3-2", "Z-", ("A", 3, 1), ("A", 3, 2), (3, 6), ["Fz3-"])
    put("Fz1+", "Z+", ("A", 1, 0), ("A", 1, 3), (4, 6), ["Fy-"])
    put("Fz1-", "Z-", ("A", 1, 0), ("A", 1, 1), (6, 8), ["Fy-"])
    put("Iz1+", "Z+", ("A", 1, 0), ("A", 1, 3), (6, 8), ["Fy-"])
    put("Iz1-", "Z-", ("A", 1, 0), ("A", 1, 1), (4, 6), ["Fy-"])
    put("Fz1+2", "Z+", ("A", 1, 3), ("A", 1, 2), (4, 6), ["Fz1+"])
    put("Fz1-2", "Z-", ("A", 1, 1), ("A", 1, 2), (6, 8), ["Fz1-"])
    upper = {3: ["Iz+"], 1: ["Gz-"], 2: ["Gz-2"]}
    lower = {3: ["Gz+"], 1: ["Iz-"], 2: ["Gz+2"]}
    for e in (3, 1, 2):
        put(f"Gy{e}+", "Y+", ("A", 0, e), ("A", 3, e), (6, 8), upper[e])
        put(f"Gy{e}-", "Y-", ("A", 0, e), ("A", 1, e), (0, 4), lower[e])
    fifth = {3: ["Iz3+"], 1: ["Fz3-"], 2: ["Fz3-2"]}
    fourth = {3: ["Fz1+"], 1: ["Iz1-"], 2: ["Fz1+2"]}
    for e in (3, 1, 2):
        put(f"Gy{e}+2", "Y+", ("A", 3, e), ("A", 2, e), (5, 8), [f"Gy{e}+"] + fifth[e])
        put(f"Gy{e}-2", "Y-", ("A", 1, e), ("A", 2, e), (4, 5), fourth[e])
    put("Fz2+", "Z+", ("A", 2, 0), ("A", 2, 3), (0, 2), ["Fy+2"])
    put("Fz2-", "Z-", ("A", 2, 0), ("A", 2, 1), (2, 4), ["Fy+2"])
    put("Iz2+", "Z+", ("A", 2, 0), ("A", 2, 3), (2, 4), ["Fy+2"])
    put("Iz2-", "Z-", ("A", 2, 0), ("A", 2, 1), (0, 2), ["Fy+2"])
    put("Fz2+2", "Z+", ("A", 2, 3), ("A", 2, 2), (0, 2), ["Fz2+"])
    put("Fz2-2", "Z-", ("A", 2, 1), ("A", 2, 2), (2, 4), ["Fz2-"])
    put("By+", "Y+", ("B", 0, 0, 0), ("B", 3, 0, 0), (0, 4), [])
    put("By-", "Y-", ("B", 0, 0, 0), ("B", 1, 0, 0), (0, 4), [])
    put("By+2", "Y+", ("B", 3, 0, 0), ("B", 2, 0, 0), (0, 2), ["By+"])
    put("By-2", "Y-", ("B", 1, 0, 0), ("B", 2, 0, 0), (2, 4), ["By-"])
    layer = {0: [], 3: ["By+"], 1: ["By-"], 2: ["By+2", "By-2"]}
    for d in ORDER:
        put(f"Bx{d}+", "X+", ("B", d, 0, 0), ("B", d, 3, 0), (0, 4), layer[d])
        put(f"Bx{d}-", "X-", ("B", d, 0, 0), ("B", d, 1, 0), (0, 4), layer[d])
        put(f"Bx{d}+2", "X+", ("B", d, 3, 0), ("B", d, 2, 0), (0, 2), [f"Bx{d}+"])
        put(f"Bx{d}-2", "X-", ("B", d, 1, 0), ("B", d, 2, 0), (2, 4), [f"Bx{d}-"])
        sources = {0: layer[d], 3: [f"Bx{d}+"], 1: [f"Bx{d}-"], 2: [f"Bx{d}+2", f"Bx{d}-2"]}
        for x, needs in sources.items():
            put(f"D{d}{x}", "D", ("B", d, x, 0), ("B", d, x, 1), (0, 4), needs)
    return out


Z_ORDER = (
    "Gz*", "Iz*", "Gz*2", "Fz3*", "Iz3*", "Fz3*2", "Fz1*", "Iz1*", "Fz1*2", "Fz2*", "Iz2*", "Fz2*2",
)
Y_ORDER = (
    "By*", "Fy*", "Hy*", "By*2", "Gy3*", "Gy1*", "Gy2*", "Fy*2", "Gy3*2", "Gy1*2", "Gy2*2",
)
X_ORDER = ("Bx0*", "Bx0*2", "Bx3*", "Bx1*", "Bx3*2", "Bx1*2", "Bx2*", "Bx2*2")


AFTER = {0: ("Gz+2", "Gz-2"), 3: ("Fz1+", "Fz1-"), 1: ("Fz2+", "Fz2-"), 2: ()}


def groups():
    out = {"By2": ("By+2", "By-2"), "Gy+": ("Gy3+", "Gy1+", "Gy2+"), "Gy-": ("Gy3-", "Gy1-", "Gy2-")}
    for d in ORDER:
        out[f"Bx{d}2"] = (f"Bx{d}+2", f"Bx{d}-2")
        out[f"D{d}"] = tuple(f"D{d}{x}" for x in range(N_X))
    grouped = {n for names in out.values() for n in names}
    out.update({n: (n,) for n in messages() if n not in grouped})
    return out


def schedule():
    table = messages()
    ready_at, free_at, waited, started, steps = {}, {}, set(), set(), []
    now = 0.0

    def send(name):
        queue, _, _, blocks, _ = table[name]
        begin = max(now, free_at.get(queue, 0.0))
        free_at[queue] = begin + (blocks[1] - blocks[0]) * (128.0 if queue == "D" else 1420.0)
        ready_at[name] = free_at[queue] + (1100.0 if queue == "D" else 2400.0)
        started.add(name)
        steps.append(("send", name))

    order = {
        axis + sign: [n.replace("*", sign) for n in names]
        for axis, names in (("Z", Z_ORDER), ("Y", Y_ORDER), ("X", X_ORDER))
        for sign in "+-"
    }

    def send_ready():
        for names in order.values():
            while names and all(n in waited for n in table[names[0]][4]):
                send(names.pop(0))
        for name, entry in table.items():
            if entry[0] == "D" and name not in started and all(n in waited for n in entry[4]):
                send(name)

    send_ready()
    steps.append(("tables",))
    now += 2500.0
    ripe = [(("A", 0, 0), (0, ACAP)), (("B", 0, 0, 0), (0, BCAP))]
    missing = {d: N_COL * ACAP + N_ROW * BCAP for d in ORDER}
    phases = list(ORDER)
    together = groups()

    def task():
        if phases and missing[phases[0]] == 0 and all(n in waited for n in AFTER[phases[0]]):
            return ("multiply", phases.pop(0)), 2900.0
        if ripe:
            slot, blocks = ripe.pop(min(range(len(ripe)), key=lambda i: ORDER.index(ripe[i][0][1])))
            missing[slot[1]] -= blocks[1] - blocks[0]
            return ("split", slot, blocks), 35.0 * (blocks[1] - blocks[0]) + 30.0
        return None

    while len(waited) < len(table) or phases:
        pending = sorted(
            (max(ready_at[n] for n in names), group)
            for group, names in together.items()
            if all(n in started for n in names) and names[0] not in waited
        )
        if pending and pending[0][0] <= now:
            group = pending[0][1]
            waited.update(together[group])
            steps.append(("wait", group))
            ripe.extend(table[n][2:4] for n in together[group])
            send_ready()
            continue
        chosen = task()
        if chosen is not None:
            steps.append(chosen[0])
            now += chosen[1]
        else:
            now = pending[0][0]
    return table, steps, now, free_at


def kernel(
    a_ref, b_ref, plan_ref, counts_ref, out_ref,
    a_land, b_land, a_half, b_half, chain, sums, plan_v, counts_v, table_v, table_s, own_sem, send_sem, recv_sem,
):
    r, c, o = lax.axis_index("row"), lax.axis_index("col"), lax.axis_index("layer")
    devices = {
        "X+": (lax.rem(r + 2, N_ROW), c, o),
        "X-": (lax.rem(r + N_ROW - 2, N_ROW), c, o),
        "D": (r + 1 - 2 * lax.rem(r, 2), c, o),
        "Y+": (r, c, lax.rem(o + 1, N_LAYER)),
        "Y-": (r, c, lax.rem(o + N_LAYER - 1, N_LAYER)),
        "Z+": (r, lax.rem(c + 1, N_COL), o),
        "Z-": (r, lax.rem(c + N_COL - 1, N_COL), o),
    }
    own = [
        pltpu.make_async_copy(a_ref, a_land.at[0, 0], own_sem.at[0]),
        pltpu.make_async_copy(b_ref, b_land.at[0, 0, 0], own_sem.at[1]),
        pltpu.make_async_copy(plan_ref, plan_v, own_sem.at[2]),
        pltpu.make_async_copy(counts_ref, counts_v, own_sem.at[3]),
    ]
    to_scalar = pltpu.make_async_copy(table_v, table_s, own_sem.at[4])
    for copy in own:
        copy.start()
    barrier = pltpu.get_barrier_semaphore()
    for device in devices.values():
        pl.semaphore_signal(barrier, inc=1, device_id=device, device_id_type=MESH)
    pl.semaphore_wait(barrier, len(devices))
    own[0].wait()
    own[1].wait()

    table, steps, _, _ = schedule()

    def view(slot, blocks):
        land = a_land if slot[0] == "A" else b_land
        return land.at[(*slot[1:], pl.ds(blocks[0], blocks[1] - blocks[0]))]

    together = groups()
    number = {n: i for i, names in enumerate(together.values()) for n in names}
    copies, sent, size = {}, [0, 0], [0] * len(together)
    for name, (queue, source, target, blocks, _) in table.items():
        pool = 0 if queue[0] in "YZ" else 1
        sent[pool] += blocks[1] - blocks[0]
        size[number[name]] += blocks[1] - blocks[0]
        copies[name] = pltpu.make_async_remote_copy(
            src_ref=view(source, blocks),
            dst_ref=view(target, blocks),
            send_sem=send_sem.at[pool],
            recv_sem=recv_sem.at[number[name]],
            device_id=devices[queue],
            device_id_type=MESH,
        )

    def make_tables():
        own[2].wait()
        own[3].wait()
        shape = (N_LAYER, PHASE)
        fields = [
            jnp.concatenate([plan_v[s, f] for s in range(LISTS)], axis=1) for f in range(3)
        ]
        limit = jnp.concatenate(
            [jnp.broadcast_to(counts_v[:, s : s + 1], (N_LAYER, PCAP)) for s in range(LISTS)], axis=1
        )
        left, right, target = fields
        at = lax.broadcasted_iota(jnp.int32, shape, 1)
        s = at // PCAP
        column = (left // (N_LAYER * ACAP) + N_COL - c) % N_COL
        x_on = (s // 2 + N_X - r // 2) % N_X
        core_on = (s + r) % 2
        live = at % PCAP < limit
        key = jnp.where(live, target, CL) * PHASE + at
        packed = (target * PHASE + column * ACAP + left % ACAP) * PHASE
        packed = packed + (x_on * 2 + core_on) * BCAP + right
        rank = jnp.zeros(shape, jnp.int32)
        for q in range(PHASE):
            rank += jnp.where(jnp.broadcast_to(key[:, q : q + 1], shape) < key, 1, 0)
        ordered, place, last = packed, target, jnp.full(shape, -1, jnp.int32)
        sort_key = key // PHASE
        for q in range(PHASE):
            here = at == jnp.broadcast_to(rank[:, q : q + 1], shape)
            ordered = jnp.where(here, jnp.broadcast_to(packed[:, q : q + 1], shape), ordered)
            place = jnp.where(here, jnp.broadcast_to(sort_key[:, q : q + 1], shape), place)
            one = jnp.broadcast_to(sort_key[:, q : q + 1], shape)
            last = jnp.where(at == one, jnp.maximum(last, jnp.broadcast_to(rank[:, q : q + 1], shape)), last)
        earlier = jnp.concatenate([place[:, 0:1] - 1, place[:, 0 : PHASE - 1]], axis=1)
        table_v[0:4] = ordered // PHASE % PHASE
        table_v[4:8] = ordered % PHASE
        table_v[8:12] = ordered // (PHASE * PHASE)
        table_v[12:16] = jnp.where(place == earlier, 0, 1)
        table_v[16:20] = jnp.where(last < 0, PHASE + at, last)

    def wait_for(sem, blocks):
        window = chain.at[pl.ds(0, blocks)]
        pltpu.make_async_copy(window, window, sem).wait()

    def split(slot, blocks):
        if slot[0] == "A":
            base, halves, land = slot[2] * ACAP, a_half, a_land
        else:
            base, halves, land = (slot[2] * 2 + slot[3]) * BCAP, b_half, b_land

        def one(block, carry):
            value = land[(*slot[1:], block)]
            high = value.astype(jnp.bfloat16)
            low = (value - high.astype(jnp.float32)).astype(jnp.bfloat16)
            halves[slot[1], base + block, :, 0:BS] = high
            halves[slot[1], base + block, :, BS : 2 * BS] = low
            return carry

        lax.fori_loop(*blocks, one, 0)

    def multiply(d, total):
        m = lax.rem(o + d, N_LAYER)
        unroll = UNROLL[d]

        def some(index, total):
            for p in range(unroll):
                at = index * unroll + p
                left = a_half[d, table_s[m, at]]
                right = b_half[d, table_s[4 + m, at]]
                both = jnp.dot(
                    left,
                    jnp.concatenate([right, right], axis=0),
                    preferred_element_type=jnp.float32,
                )
                first = jnp.broadcast_to(table_s[12 + m, at], (BS, BS)) == 1
                total = jnp.where(first, sums[table_s[8 + m, at]], total)
                total = total + (both[:, 0:BS] + both[:, BS : 2 * BS])
                chain[at] = total
            return total

        return lax.fori_loop(0, PHASE // unroll, some, total)

    def collect(d):
        m = lax.rem(o + d, N_LAYER)

        def one(t, carry):
            at = table_s[16 + m, t]
            total = jnp.where(
                jnp.broadcast_to(at, (BS, BS)) < PHASE, chain[jnp.minimum(at, PHASE - 1)], sums[t]
            )
            if d == ORDER[-1]:
                out_ref[t] = total
            else:
                sums[t] = total
            return carry

        lax.fori_loop(0, CL, one, 0)

    def clear(t, carry):
        sums[t] = jnp.zeros((BS, BS), jnp.float32)
        return carry

    scalars, running = "none", jnp.zeros((BS, BS), jnp.float32)
    for step in steps:
        if step[0] == "send":
            copies[step[1]].start()
        elif step[0] == "tables":
            make_tables()
            lax.fori_loop(0, CL, clear, 0)
        elif step[0] == "wait":
            names = together[step[1]]
            if len(names) == 1:
                copies[names[0]].wait_recv()
            else:
                wait_for(recv_sem.at[number[names[0]]], size[number[names[0]]])
            if scalars == "none":
                to_scalar.start()
                scalars = "started"
        elif step[0] == "split":
            split(*step[1:])
        else:
            if scalars == "started":
                to_scalar.wait()
                scalars = "there"
            running = multiply(step[1], running)
            collect(step[1])
    for pool in range(2):
        wait_for(send_sem.at[pool], sent[pool])


def per_device(a_blocks, b_blocks, pair_plan, pair_counts):
    count = len(groups())
    hbm = pl.BlockSpec(memory_space=pltpu.HBM)
    plan = pair_plan[0, 0, 0].transpose(0, 2, 1, 3)
    operands = (a_blocks[0], b_blocks[:, 0], plan, pair_counts[0, 0, 0].T)
    result = pl.pallas_call(
        kernel,
        out_shape=jax.ShapeDtypeStruct((CL, BS, BS), jnp.float32),
        in_specs=[hbm, hbm, hbm, hbm],
        out_specs=pl.BlockSpec(memory_space=pltpu.VMEM),
        scratch_shapes=[
            pltpu.VMEM((N_LAYER, N_COL, ACAP, BS, BS), jnp.float32),
            pltpu.VMEM((N_LAYER, N_X, 2, BCAP, BS, BS), jnp.float32),
            pltpu.VMEM((N_LAYER, N_COL * ACAP, BS, 2 * BS), jnp.bfloat16),
            pltpu.VMEM((N_LAYER, N_ROW * BCAP, BS, 2 * BS), jnp.bfloat16),
            pltpu.VMEM((PHASE + BCAP, BS, BS), jnp.float32),
            pltpu.VMEM((CL, BS, BS), jnp.float32),
            pltpu.VMEM((N_ROW, 3, N_LAYER, PCAP), jnp.int32),
            pltpu.VMEM((N_LAYER, N_ROW), jnp.int32),
            pltpu.VMEM((24, PHASE), jnp.int32),
            pltpu.SMEM((24, PHASE), jnp.int32),
            pltpu.SemaphoreType.DMA((5,)),
            pltpu.SemaphoreType.DMA((2,)),
            pltpu.SemaphoreType.DMA((count,)),
        ],
        compiler_params=pltpu.CompilerParams(
            collective_id=0, has_side_effects=True, vmem_limit_bytes=50 * 1024 * 1024
        ),
        name="gather_multiply",
    )(*[pltpu.with_memory_space_constraint(x, pltpu.HBM) for x in operands])
    return result[None, None]


def solution(mesh):
    in_specs = (
        P("row", ("col", "layer"), None, None),
        P(("row", "layer"), "col", None, None),
        P("row", "col", "layer", None, None, None, None),
        P("row", "col", "layer", None, None),
    )
    out_specs = P("row", "col", "layer", None, None)
    return jax.shard_map(
        per_device, mesh=mesh, in_specs=in_specs, out_specs=out_specs, check_vma=False
    )
```

```python
import jax
import jax.numpy as jnp
from jax import lax
from jax.experimental import pallas as pl
from jax.experimental.pallas import tpu as pltpu
from jax.sharding import PartitionSpec as P

BS = 128
ACAP = 8
BCAP = 4
PCAP = 16
CL = 32
N_ROW, N_COL, N_LAYER = 8, 4, 4
N_X = N_ROW // 2
LISTS = N_ROW
PHASE = LISTS * PCAP
UNROLL = {0: 32, 3: 32, 1: 32, 2: 128}
ORDER = (0, 3, 1, 2)
MESH = pl.DeviceIdType.MESH


def messages():
    out = {}

    def put(name, *entry):
        out[name] = entry

    put("Fy+", "Y+", ("A", 0, 0), ("A", 3, 0), (0, 6), [])
    put("Fy-", "Y-", ("A", 0, 0), ("A", 1, 0), (4, 8), [])
    put("Hy+", "Y+", ("A", 0, 0), ("A", 3, 0), (6, 8), [])
    put("Hy-", "Y-", ("A", 0, 0), ("A", 1, 0), (0, 4), [])
    put("Fy+2", "Y+", ("A", 3, 0), ("A", 2, 0), (0, 4), ["Fy+"])
    put("Fy-2", "Y-", ("A", 1, 0), ("A", 2, 0), (4, 8), ["Fy-"])
    put("Gz+", "Z+", ("A", 0, 0), ("A", 0, 3), (0, 4), [])
    put("Gz-", "Z-", ("A", 0, 0), ("A", 0, 1), (4, 8), [])
    put("Iz+", "Z+", ("A", 0, 0), ("A", 0, 3), (4, 8), [])
    put("Iz-", "Z-", ("A", 0, 0), ("A", 0, 1), (0, 4), [])
    put("Gz+2", "Z+", ("A", 0, 3), ("A", 0, 2), (0, 4), ["Gz+"])
    put("Gz-2", "Z-", ("A", 0, 1), ("A", 0, 2), (4, 8), ["Gz-"])
    put("Fz3+", "Z+", ("A", 3, 0), ("A", 3, 3), (0, 3), ["Fy+"])
    put("Fz3-", "Z-", ("A", 3, 0), ("A", 3, 1), (3, 6), ["Fy+"])
    put("Iz3+", "Z+", ("A", 3, 0), ("A", 3, 3), (3, 6), ["Fy+"])
    put("Iz3-", "Z-", ("A", 3, 0), ("A", 3, 1), (0, 3), ["Fy+"])
    put("Fz3+2", "Z+", ("A", 3, 3), ("A", 3, 2), (0, 3), ["Fz3+"])
    put("Fz3-2", "Z-", ("A", 3, 1), ("A", 3, 2), (3, 6), ["Fz3-"])
    put("Fz1+", "Z+", ("A", 1, 0), ("A", 1, 3), (4, 6), ["Fy-"])
    put("Fz1-", "Z-", ("A", 1, 0), ("A", 1, 1), (6, 8), ["Fy-"])
    put("Iz1+", "Z+", ("A", 1, 0), ("A", 1, 3), (6, 8), ["Fy-"])
    put("Iz1-", "Z-", ("A", 1, 0), ("A", 1, 1), (4, 6), ["Fy-"])
    put("Fz1+2", "Z+", ("A", 1, 3), ("A", 1, 2), (4, 6), ["Fz1+"])
    put("Fz1-2", "Z-", ("A", 1, 1), ("A", 1, 2), (6, 8), ["Fz1-"])
    upper = {3: ["Iz+"], 1: ["Gz-"], 2: ["Gz-2"]}
    lower = {3: ["Gz+"], 1: ["Iz-"], 2: ["Gz+2"]}
    for e in (3, 1, 2):
        put(f"Gy{e}+", "Y+", ("A", 0, e), ("A", 3, e), (6, 8), upper[e])
        put(f"Gy{e}-", "Y-", ("A", 0, e), ("A", 1, e), (0, 4), lower[e])
    fifth = {3: ["Iz3+"], 1: ["Fz3-"], 2: ["Fz3-2"]}
    fourth = {3: ["Fz1+"], 1: ["Iz1-"], 2: ["Fz1+2"]}
    for e in (3, 1, 2):
        put(f"Gy{e}+2", "Y+", ("A", 3, e), ("A", 2, e), (5, 8), [f"Gy{e}+"] + fifth[e])
        put(f"Gy{e}-2", "Y-", ("A", 1, e), ("A", 2, e), (4, 5), fourth[e])
    put("Fz2+", "Z+", ("A", 2, 0), ("A", 2, 3), (0, 2), ["Fy+2"])
    put("Fz2-", "Z-", ("A", 2, 0), ("A", 2, 1), (2, 4), ["Fy+2"])
    put("Iz2+", "Z+", ("A", 2, 0), ("A", 2, 3), (2, 4), ["Fy+2"])
    put("Iz2-", "Z-", ("A", 2, 0), ("A", 2, 1), (0, 2), ["Fy+2"])
    put("Fz2+2", "Z+", ("A", 2, 3), ("A", 2, 2), (0, 2), ["Fz2+"])
    put("Fz2-2", "Z-", ("A", 2, 1), ("A", 2, 2), (2, 4), ["Fz2-"])
    put("By+", "Y+", ("B", 0, 0, 0), ("B", 3, 0, 0), (0, 4), [])
    put("By-", "Y-", ("B", 0, 0, 0), ("B", 1, 0, 0), (0, 4), [])
    put("By+2", "Y+", ("B", 3, 0, 0), ("B", 2, 0, 0), (0, 2), ["By+"])
    put("By-2", "Y-", ("B", 1, 0, 0), ("B", 2, 0, 0), (2, 4), ["By-"])
    layer = {0: [], 3: ["By+"], 1: ["By-"], 2: ["By+2", "By-2"]}
    for d in ORDER:
        put(f"Bx{d}+", "X+", ("B", d, 0, 0), ("B", d, 3, 0), (0, 4), layer[d])
        put(f"Bx{d}-", "X-", ("B", d, 0, 0), ("B", d, 1, 0), (0, 4), layer[d])
        put(f"Bx{d}+2", "X+", ("B", d, 3, 0), ("B", d, 2, 0), (0, 2), [f"Bx{d}+"])
        put(f"Bx{d}-2", "X-", ("B", d, 1, 0), ("B", d, 2, 0), (2, 4), [f"Bx{d}-"])
        sources = {0: layer[d], 3: [f"Bx{d}+"], 1: [f"Bx{d}-"], 2: [f"Bx{d}+2", f"Bx{d}-2"]}
        for x, needs in sources.items():
            put(f"D{d}{x}", "D", ("B", d, x, 0), ("B", d, x, 1), (0, 4), needs)
    return out


Z_ORDER = (
    "Gz*", "Iz*", "Gz*2", "Fz3*", "Iz3*", "Fz3*2", "Fz1*", "Iz1*", "Fz1*2", "Fz2*", "Iz2*", "Fz2*2",
)
Y_ORDER = (
    "By*", "Fy*", "Hy*", "By*2", "Gy3*", "Gy1*", "Gy2*", "Fy*2", "Gy3*2", "Gy1*2", "Gy2*2",
)
X_ORDER = ("Bx0*", "Bx0*2", "Bx3*", "Bx1*", "Bx3*2", "Bx1*2", "Bx2*", "Bx2*2")


AFTER = {0: ("Gz+2", "Gz-2"), 3: ("Fz1+", "Fz1-"), 1: ("Fz2+", "Fz2-"), 2: ()}


def groups():
    out = {"By2": ("By+2", "By-2"), "Gy+": ("Gy3+", "Gy1+", "Gy2+"), "Gy-": ("Gy3-", "Gy1-", "Gy2-")}
    for d in ORDER:
        out[f"Bx{d}2"] = (f"Bx{d}+2", f"Bx{d}-2")
        out[f"D{d}"] = tuple(f"D{d}{x}" for x in range(N_X))
    grouped = {n for names in out.values() for n in names}
    out.update({n: (n,) for n in messages() if n not in grouped})
    return out


def schedule():
    table = messages()
    ready_at, free_at, waited, started, steps = {}, {}, set(), set(), []
    now = 0.0

    def send(name):
        queue, _, _, blocks, _ = table[name]
        begin = max(now, free_at.get(queue, 0.0))
        free_at[queue] = begin + (blocks[1] - blocks[0]) * (128.0 if queue == "D" else 1420.0)
        ready_at[name] = free_at[queue] + (1100.0 if queue == "D" else 2400.0)
        started.add(name)
        steps.append(("send", name))

    order = {
        axis + sign: [n.replace("*", sign) for n in names]
        for axis, names in (("Z", Z_ORDER), ("Y", Y_ORDER), ("X", X_ORDER))
        for sign in "+-"
    }

    def send_ready():
        for names in order.values():
            while names and all(n in waited for n in table[names[0]][4]):
                send(names.pop(0))
        for name, entry in table.items():
            if entry[0] == "D" and name not in started and all(n in waited for n in entry[4]):
                send(name)

    send_ready()
    steps.append(("tables",))
    now += 2500.0
    ripe = [(("A", 0, 0), (0, ACAP)), (("B", 0, 0, 0), (0, BCAP))]
    missing = {d: N_COL * ACAP + N_ROW * BCAP for d in ORDER}
    phases = list(ORDER)
    together = groups()

    def task():
        if phases and missing[phases[0]] == 0 and all(n in waited for n in AFTER[phases[0]]):
            return ("multiply", phases.pop(0)), 2900.0
        if ripe:
            slot, blocks = ripe.pop(min(range(len(ripe)), key=lambda i: ORDER.index(ripe[i][0][1])))
            missing[slot[1]] -= blocks[1] - blocks[0]
            return ("split", slot, blocks), 35.0 * (blocks[1] - blocks[0]) + 30.0
        return None

    while len(waited) < len(table) or phases:
        pending = sorted(
            (max(ready_at[n] for n in names), group)
            for group, names in together.items()
            if all(n in started for n in names) and names[0] not in waited
        )
        if pending and pending[0][0] <= now:
            group = pending[0][1]
            waited.update(together[group])
            steps.append(("wait", group))
            ripe.extend(table[n][2:4] for n in together[group])
            send_ready()
            continue
        chosen = task()
        if chosen is not None:
            steps.append(chosen[0])
            now += chosen[1]
        else:
            now = pending[0][0]
    return table, steps, now, free_at


def kernel(
    a_ref, b_ref, plan_ref, counts_ref, out_ref,
    a_land, b_land, a_half, b_half, chain, sums, plan_v, counts_v, table_v, table_s, own_sem, send_sem, recv_sem,
):
    r, c, o = lax.axis_index("row"), lax.axis_index("col"), lax.axis_index("layer")
    devices = {
        "X+": (lax.rem(r + 2, N_ROW), c, o),
        "X-": (lax.rem(r + N_ROW - 2, N_ROW), c, o),
        "D": (r + 1 - 2 * lax.rem(r, 2), c, o),
        "Y+": (r, c, lax.rem(o + 1, N_LAYER)),
        "Y-": (r, c, lax.rem(o + N_LAYER - 1, N_LAYER)),
        "Z+": (r, lax.rem(c + 1, N_COL), o),
        "Z-": (r, lax.rem(c + N_COL - 1, N_COL), o),
    }
    own = [
        pltpu.make_async_copy(a_ref, a_land.at[0, 0], own_sem.at[0]),
        pltpu.make_async_copy(b_ref, b_land.at[0, 0, 0], own_sem.at[1]),
        pltpu.make_async_copy(plan_ref, plan_v, own_sem.at[2]),
        pltpu.make_async_copy(counts_ref, counts_v, own_sem.at[3]),
    ]
    to_scalar = pltpu.make_async_copy(table_v, table_s, own_sem.at[4])
    for copy in own:
        copy.start()
    barrier = pltpu.get_barrier_semaphore()
    for device in devices.values():
        pl.semaphore_signal(barrier, inc=1, device_id=device, device_id_type=MESH)
    pl.semaphore_wait(barrier, len(devices))
    own[0].wait()
    own[1].wait()

    table, steps, _, _ = schedule()

    def view(slot, blocks):
        land = a_land if slot[0] == "A" else b_land
        return land.at[(*slot[1:], pl.ds(blocks[0], blocks[1] - blocks[0]))]

    together = groups()
    number = {n: i for i, names in enumerate(together.values()) for n in names}
    copies, sent, size = {}, [0, 0], [0] * len(together)
    for name, (queue, source, target, blocks, _) in table.items():
        pool = 0 if queue[0] in "YZ" else 1
        sent[pool] += blocks[1] - blocks[0]
        size[number[name]] += blocks[1] - blocks[0]
        copies[name] = pltpu.make_async_remote_copy(
            src_ref=view(source, blocks),
            dst_ref=view(target, blocks),
            send_sem=send_sem.at[pool],
            recv_sem=recv_sem.at[number[name]],
            device_id=devices[queue],
            device_id_type=MESH,
        )

    def make_tables():
        own[2].wait()
        own[3].wait()
        shape = (N_LAYER, PHASE)
        fields = [
            jnp.concatenate([plan_v[s, f] for s in range(LISTS)], axis=1) for f in range(3)
        ]
        limit = jnp.concatenate(
            [jnp.broadcast_to(counts_v[:, s : s + 1], (N_LAYER, PCAP)) for s in range(LISTS)], axis=1
        )
        left, right, target = fields
        at = lax.broadcasted_iota(jnp.int32, shape, 1)
        s = at // PCAP
        column = (left // (N_LAYER * ACAP) + N_COL - c) % N_COL
        x_on = (s // 2 + N_X - r // 2) % N_X
        core_on = (s + r) % 2
        live = at % PCAP < limit
        key = jnp.where(live, target, CL) * PHASE + at
        packed = (target * PHASE + column * ACAP + left % ACAP) * PHASE
        packed = packed + (x_on * 2 + core_on) * BCAP + right
        rank = jnp.zeros(shape, jnp.int32)
        for q in range(PHASE):
            rank += jnp.where(jnp.broadcast_to(key[:, q : q + 1], shape) < key, 1, 0)
        ordered, place, last = packed, target, jnp.full(shape, -1, jnp.int32)
        sort_key = key // PHASE
        for q in range(PHASE):
            here = at == jnp.broadcast_to(rank[:, q : q + 1], shape)
            ordered = jnp.where(here, jnp.broadcast_to(packed[:, q : q + 1], shape), ordered)
            place = jnp.where(here, jnp.broadcast_to(sort_key[:, q : q + 1], shape), place)
            one = jnp.broadcast_to(sort_key[:, q : q + 1], shape)
            last = jnp.where(at == one, jnp.maximum(last, jnp.broadcast_to(rank[:, q : q + 1], shape)), last)
        earlier = jnp.concatenate([place[:, 0:1] - 1, place[:, 0 : PHASE - 1]], axis=1)
        table_v[0:4] = ordered // PHASE % PHASE
        table_v[4:8] = ordered % PHASE
        table_v[8:12] = ordered // (PHASE * PHASE)
        table_v[12:16] = jnp.where(place == earlier, 0, 1)
        table_v[16:20] = jnp.where(last < 0, PHASE + at, last)

    def wait_for(sem, blocks):
        window = chain.at[pl.ds(0, blocks)]
        pltpu.make_async_copy(window, window, sem).wait()

    def split(slot, blocks):
        if slot[0] == "A":
            base, halves, land = slot[2] * ACAP, a_half, a_land
        else:
            base, halves, land = (slot[2] * 2 + slot[3]) * BCAP, b_half, b_land

        def one(block):
            value = land[(*slot[1:], block)]
            high = value.astype(jnp.bfloat16)
            low = (value - high.astype(jnp.float32)).astype(jnp.bfloat16)
            halves[slot[1], base + block, :, 0:BS] = high
            halves[slot[1], base + block, :, BS : 2 * BS] = low

        def two(step, carry):
            one(blocks[0] + 2 * step)
            one(blocks[0] + 2 * step + 1)
            return carry

        pairs, odd = divmod(blocks[1] - blocks[0], 2)
        lax.fori_loop(0, pairs, two, 0)
        if odd:
            one(blocks[1] - 1)

    def multiply(d, total):
        m = lax.rem(o + d, N_LAYER)
        unroll = UNROLL[d]

        def some(index, total):
            for p in range(unroll):
                at = index * unroll + p
                left = a_half[d, table_s[m, at]]
                right = b_half[d, table_s[4 + m, at]]
                both = jnp.dot(
                    left,
                    jnp.concatenate([right, right], axis=0),
                    preferred_element_type=jnp.float32,
                )
                first = jnp.broadcast_to(table_s[12 + m, at], (BS, BS)) == 1
                total = jnp.where(first, sums[table_s[8 + m, at]], total)
                total = total + (both[:, 0:BS] + both[:, BS : 2 * BS])
                chain[at] = total
            return total

        return lax.fori_loop(0, PHASE // unroll, some, total)

    def collect(d):
        m = lax.rem(o + d, N_LAYER)

        def some(step, carry):
            for k in range(4):
                t = step * 4 + k
                total = chain[table_s[16 + m, t]]
                if d == ORDER[-1]:
                    out_ref[t] = total
                else:
                    sums[t] = total
                    chain[PHASE + t] = total
            return carry

        lax.fori_loop(0, CL // 4, some, 0)

    def clear(t, carry):
        sums[t] = jnp.zeros((BS, BS), jnp.float32)
        chain[PHASE + t] = jnp.zeros((BS, BS), jnp.float32)
        return carry

    scalars, running = "none", jnp.zeros((BS, BS), jnp.float32)
    for step in steps:
        if step[0] == "send":
            copies[step[1]].start()
        elif step[0] == "tables":
            make_tables()
            lax.fori_loop(0, CL, clear, 0)
        elif step[0] == "wait":
            names = together[step[1]]
            if len(names) == 1:
                copies[names[0]].wait_recv()
            else:
                wait_for(recv_sem.at[number[names[0]]], size[number[names[0]]])
            if scalars == "none":
                to_scalar.start()
                scalars = "started"
        elif step[0] == "split":
            split(*step[1:])
        else:
            if scalars == "started":
                to_scalar.wait()
                scalars = "there"
            running = multiply(step[1], running)
            collect(step[1])
    for pool in range(2):
        wait_for(send_sem.at[pool], sent[pool])


def per_device(a_blocks, b_blocks, pair_plan, pair_counts):
    count = len(groups())
    hbm = pl.BlockSpec(memory_space=pltpu.HBM)
    plan = pair_plan[0, 0, 0].transpose(0, 2, 1, 3)
    operands = (a_blocks[0], b_blocks[:, 0], plan, pair_counts[0, 0, 0].T)
    result = pl.pallas_call(
        kernel,
        out_shape=jax.ShapeDtypeStruct((CL, BS, BS), jnp.float32),
        in_specs=[hbm, hbm, hbm, hbm],
        out_specs=pl.BlockSpec(memory_space=pltpu.VMEM),
        scratch_shapes=[
            pltpu.VMEM((N_LAYER, N_COL, ACAP, BS, BS), jnp.float32),
            pltpu.VMEM((N_LAYER, N_X, 2, BCAP, BS, BS), jnp.float32),
            pltpu.VMEM((N_LAYER, N_COL * ACAP, BS, 2 * BS), jnp.bfloat16),
            pltpu.VMEM((N_LAYER, N_ROW * BCAP, BS, 2 * BS), jnp.bfloat16),
            pltpu.VMEM((PHASE + CL, BS, BS), jnp.float32),
            pltpu.VMEM((CL, BS, BS), jnp.float32),
            pltpu.VMEM((N_ROW, 3, N_LAYER, PCAP), jnp.int32),
            pltpu.VMEM((N_LAYER, N_ROW), jnp.int32),
            pltpu.VMEM((24, PHASE), jnp.int32),
            pltpu.SMEM((24, PHASE), jnp.int32),
            pltpu.SemaphoreType.DMA((5,)),
            pltpu.SemaphoreType.DMA((2,)),
            pltpu.SemaphoreType.DMA((count,)),
        ],
        compiler_params=pltpu.CompilerParams(
            collective_id=0, has_side_effects=True, vmem_limit_bytes=50 * 1024 * 1024
        ),
        name="gather_multiply",
    )(*[pltpu.with_memory_space_constraint(x, pltpu.HBM) for x in operands])
    return result[None, None]


def solution(mesh):
    in_specs = (
        P("row", ("col", "layer"), None, None),
        P(("row", "layer"), "col", None, None),
        P("row", "col", "layer", None, None, None, None),
        P("row", "col", "layer", None, None),
    )
    out_specs = P("row", "col", "layer", None, None)
    return jax.shard_map(
        per_device, mesh=mesh, in_specs=in_specs, out_specs=out_specs, check_vma=False
    )
```

```python
import jax
import jax.numpy as jnp
from jax import lax
from jax.experimental import pallas as pl
from jax.experimental.pallas import tpu as pltpu
from jax.sharding import PartitionSpec as P

BS = 128
ACAP = 8
BCAP = 4
PCAP = 16
CL = 32
N_ROW, N_COL, N_LAYER = 8, 4, 4
N_X = N_ROW // 2
LISTS = N_ROW
PHASE = LISTS * PCAP
UNROLL = {0: 32, 3: 32, 1: 32, 2: 128}
ORDER = (0, 3, 1, 2)
MESH = pl.DeviceIdType.MESH


def messages():
    out = {}

    def put(name, *entry):
        out[name] = entry

    put("Fy+", "Y+", ("A", 0, 0), ("A", 3, 0), (0, 6), [])
    put("Fy-", "Y-", ("A", 0, 0), ("A", 1, 0), (4, 8), [])
    put("Hy+", "Y+", ("A", 0, 0), ("A", 3, 0), (6, 8), [])
    put("Hy-", "Y-", ("A", 0, 0), ("A", 1, 0), (0, 4), [])
    put("Fy+2", "Y+", ("A", 3, 0), ("A", 2, 0), (0, 4), ["Fy+"])
    put("Fy-2", "Y-", ("A", 1, 0), ("A", 2, 0), (4, 8), ["Fy-"])
    put("Gz+", "Z+", ("A", 0, 0), ("A", 0, 3), (0, 4), [])
    put("Gz-", "Z-", ("A", 0, 0), ("A", 0, 1), (4, 8), [])
    put("Iz+", "Z+", ("A", 0, 0), ("A", 0, 3), (4, 8), [])
    put("Iz-", "Z-", ("A", 0, 0), ("A", 0, 1), (0, 4), [])
    put("Gz+2", "Z+", ("A", 0, 3), ("A", 0, 2), (0, 4), ["Gz+"])
    put("Gz-2", "Z-", ("A", 0, 1), ("A", 0, 2), (4, 8), ["Gz-"])
    put("Fz3+", "Z+", ("A", 3, 0), ("A", 3, 3), (0, 3), ["Fy+"])
    put("Fz3-", "Z-", ("A", 3, 0), ("A", 3, 1), (3, 6), ["Fy+"])
    put("Iz3+", "Z+", ("A", 3, 0), ("A", 3, 3), (3, 6), ["Fy+"])
    put("Iz3-", "Z-", ("A", 3, 0), ("A", 3, 1), (0, 3), ["Fy+"])
    put("Fz3+2", "Z+", ("A", 3, 3), ("A", 3, 2), (0, 3), ["Fz3+"])
    put("Fz3-2", "Z-", ("A", 3, 1), ("A", 3, 2), (3, 6), ["Fz3-"])
    put("Fz1+", "Z+", ("A", 1, 0), ("A", 1, 3), (4, 6), ["Fy-"])
    put("Fz1-", "Z-", ("A", 1, 0), ("A", 1, 1), (6, 8), ["Fy-"])
    put("Iz1+", "Z+", ("A", 1, 0), ("A", 1, 3), (6, 8), ["Fy-"])
    put("Iz1-", "Z-", ("A", 1, 0), ("A", 1, 1), (4, 6), ["Fy-"])
    put("Fz1+2", "Z+", ("A", 1, 3), ("A", 1, 2), (4, 6), ["Fz1+"])
    put("Fz1-2", "Z-", ("A", 1, 1), ("A", 1, 2), (6, 8), ["Fz1-"])
    upper = {3: ["Iz+"], 1: ["Gz-"], 2: ["Gz-2"]}
    lower = {3: ["Gz+"], 1: ["Iz-"], 2: ["Gz+2"]}
    for e in (3, 1, 2):
        put(f"Gy{e}+", "Y+", ("A", 0, e), ("A", 3, e), (6, 8), upper[e])
        put(f"Gy{e}-", "Y-", ("A", 0, e), ("A", 1, e), (0, 4), lower[e])
    fifth = {3: ["Iz3+"], 1: ["Fz3-"], 2: ["Fz3-2"]}
    fourth = {3: ["Fz1+"], 1: ["Iz1-"], 2: ["Fz1+2"]}
    for e in (3, 1, 2):
        stop = 7 if e == 2 else 8
        put(f"Gy{e}+2", "Y+", ("A", 3, e), ("A", 2, e), (5, stop), [f"Gy{e}+"] + fifth[e])
        put(f"Gy{e}-2", "Y-", ("A", 1, e), ("A", 2, e), (4, 5), fourth[e])
    put("Fz2+", "Z+", ("A", 2, 0), ("A", 2, 3), (0, 2), ["Fy+2"])
    put("Fz2-", "Z-", ("A", 2, 0), ("A", 2, 1), (2, 4), ["Fy+2"])
    put("Iz2+", "Z+", ("A", 2, 0), ("A", 2, 3), (2, 4), ["Fy+2"])
    put("Iz2-", "Z-", ("A", 2, 0), ("A", 2, 1), (0, 2), ["Fy+2"])
    put("Jy2+2", "Y+", ("A", 3, 2), ("A", 2, 2), (7, 8), ["Gy2+"])
    put("Fz2+2", "Z+", ("A", 2, 3), ("A", 2, 2), (0, 1), ["Fz2+"])
    put("Fz2-2", "Z-", ("A", 2, 1), ("A", 2, 2), (2, 3), ["Fz2-"])
    put("Jz2+2", "Z+", ("A", 2, 3), ("A", 2, 2), (1, 2), ["Fz2+"])
    put("Jz2-2", "Z-", ("A", 2, 1), ("A", 2, 2), (3, 4), ["Fz2-"])
    put("By+", "Y+", ("B", 0, 0, 0), ("B", 3, 0, 0), (0, 4), [])
    put("By-", "Y-", ("B", 0, 0, 0), ("B", 1, 0, 0), (0, 4), [])
    put("By+2", "Y+", ("B", 3, 0, 0), ("B", 2, 0, 0), (0, 2), ["By+"])
    put("By-2", "Y-", ("B", 1, 0, 0), ("B", 2, 0, 0), (2, 4), ["By-"])
    layer = {0: [], 3: ["By+"], 1: ["By-"], 2: ["By+2", "By-2"]}
    for d in ORDER:
        put(f"Bx{d}+", "X+", ("B", d, 0, 0), ("B", d, 3, 0), (0, 4), layer[d])
        put(f"Bx{d}-", "X-", ("B", d, 0, 0), ("B", d, 1, 0), (0, 4), layer[d])
        put(f"Bx{d}+2", "X+", ("B", d, 3, 0), ("B", d, 2, 0), (0, 2), [f"Bx{d}+"])
        put(f"Bx{d}-2", "X-", ("B", d, 1, 0), ("B", d, 2, 0), (2, 4), [f"Bx{d}-"])
        sources = {0: layer[d], 3: [f"Bx{d}+"], 1: [f"Bx{d}-"], 2: [f"Bx{d}+2", f"Bx{d}-2"]}
        for x, needs in sources.items():
            put(f"D{d}{x}", "D", ("B", d, x, 0), ("B", d, x, 1), (0, 4), needs)
    return out


Z_ORDER = (
    "Gz*", "Iz*", "Gz*2", "Fz3*", "Iz3*", "Fz3*2", "Fz1*", "Iz1*", "Fz1*2", "Fz2*", "Iz2*", "Fz2*2", "Jz2*2",
)
Y_ORDER = (
    "By*", "Fy*", "Hy*", "By*2", "Gy3*", "Gy1*", "Gy2*", "Fy*2", "Gy3*2", "Gy1*2", "Gy2*2", "Jy2*2",
)
X_ORDER = ("Bx0*", "Bx0*2", "Bx3*", "Bx1*", "Bx3*2", "Bx1*2", "Bx2*", "Bx2*2")


AFTER = {0: ("Gz+2", "Gz-2"), 3: ("Fz1+", "Fz1-"), 1: ("Fz2+", "Fz2-"), 2: ()}


def groups():
    out = {"By2": ("By+2", "By-2"), "Gy+": ("Gy3+", "Gy1+", "Gy2+"), "Gy-": ("Gy3-", "Gy1-", "Gy2-")}
    for d in ORDER:
        out[f"Bx{d}2"] = (f"Bx{d}+2", f"Bx{d}-2")
        out[f"D{d}"] = tuple(f"D{d}{x}" for x in range(N_X))
    grouped = {n for names in out.values() for n in names}
    out.update({n: (n,) for n in messages() if n not in grouped})
    return out


def schedule():
    table = messages()
    ready_at, free_at, waited, started, steps = {}, {}, set(), set(), []
    now = 0.0

    def send(name):
        queue, _, _, blocks, _ = table[name]
        begin = max(now, free_at.get(queue, 0.0))
        free_at[queue] = begin + (blocks[1] - blocks[0]) * (128.0 if queue == "D" else 1420.0)
        ready_at[name] = free_at[queue] + (1100.0 if queue == "D" else 2400.0)
        started.add(name)
        steps.append(("send", name))

    order = {
        axis + sign: [n.replace("*", sign) for n in names if n.replace("*", sign) in table]
        for axis, names in (("Z", Z_ORDER), ("Y", Y_ORDER), ("X", X_ORDER))
        for sign in "+-"
    }

    def send_ready():
        for names in order.values():
            while names and all(n in waited for n in table[names[0]][4]):
                send(names.pop(0))
        for name, entry in table.items():
            if entry[0] == "D" and name not in started and all(n in waited for n in entry[4]):
                send(name)

    send_ready()
    steps.append(("tables",))
    now += 2500.0
    ripe = [(("A", 0, 0), (0, ACAP)), (("B", 0, 0, 0), (0, BCAP))]
    missing = {d: N_COL * ACAP + N_ROW * BCAP for d in ORDER}
    phases = list(ORDER)
    together = groups()

    def task():
        if phases and missing[phases[0]] == 0 and all(n in waited for n in AFTER[phases[0]]):
            return ("multiply", phases.pop(0)), 2900.0
        if ripe:
            slot, blocks = ripe.pop(min(range(len(ripe)), key=lambda i: ORDER.index(ripe[i][0][1])))
            missing[slot[1]] -= blocks[1] - blocks[0]
            return ("split", slot, blocks), 35.0 * (blocks[1] - blocks[0]) + 30.0
        return None

    while len(waited) < len(table) or phases:
        pending = sorted(
            (max(ready_at[n] for n in names), group)
            for group, names in together.items()
            if all(n in started for n in names) and names[0] not in waited
        )
        if pending and pending[0][0] <= now:
            group = pending[0][1]
            waited.update(together[group])
            steps.append(("wait", group))
            ripe.extend(table[n][2:4] for n in together[group])
            send_ready()
            continue
        chosen = task()
        if chosen is not None:
            steps.append(chosen[0])
            now += chosen[1]
        else:
            now = pending[0][0]
    return table, steps, now, free_at


def kernel(
    a_ref, b_ref, plan_ref, counts_ref, out_ref,
    a_land, b_land, a_half, b_half, chain, sums, plan_v, counts_v, table_v, table_s, own_sem, send_sem, recv_sem,
):
    r, c, o = lax.axis_index("row"), lax.axis_index("col"), lax.axis_index("layer")
    devices = {
        "X+": (lax.rem(r + 2, N_ROW), c, o),
        "X-": (lax.rem(r + N_ROW - 2, N_ROW), c, o),
        "D": (r + 1 - 2 * lax.rem(r, 2), c, o),
        "Y+": (r, c, lax.rem(o + 1, N_LAYER)),
        "Y-": (r, c, lax.rem(o + N_LAYER - 1, N_LAYER)),
        "Z+": (r, lax.rem(c + 1, N_COL), o),
        "Z-": (r, lax.rem(c + N_COL - 1, N_COL), o),
    }
    own = [
        pltpu.make_async_copy(a_ref, a_land.at[0, 0], own_sem.at[0]),
        pltpu.make_async_copy(b_ref, b_land.at[0, 0, 0], own_sem.at[1]),
        pltpu.make_async_copy(plan_ref, plan_v, own_sem.at[2]),
        pltpu.make_async_copy(counts_ref, counts_v, own_sem.at[3]),
    ]
    to_scalar = pltpu.make_async_copy(table_v, table_s, own_sem.at[4])
    for copy in own:
        copy.start()
    barrier = pltpu.get_barrier_semaphore()
    for device in devices.values():
        pl.semaphore_signal(barrier, inc=1, device_id=device, device_id_type=MESH)
    pl.semaphore_wait(barrier, len(devices))
    own[0].wait()
    own[1].wait()

    table, steps, _, _ = schedule()

    def view(slot, blocks):
        land = a_land if slot[0] == "A" else b_land
        return land.at[(*slot[1:], pl.ds(blocks[0], blocks[1] - blocks[0]))]

    together = groups()
    number = {n: i for i, names in enumerate(together.values()) for n in names}
    copies, sent, size = {}, [0, 0], [0] * len(together)
    for name, (queue, source, target, blocks, _) in table.items():
        pool = 0 if queue[0] in "YZ" else 1
        sent[pool] += blocks[1] - blocks[0]
        size[number[name]] += blocks[1] - blocks[0]
        copies[name] = pltpu.make_async_remote_copy(
            src_ref=view(source, blocks),
            dst_ref=view(target, blocks),
            send_sem=send_sem.at[pool],
            recv_sem=recv_sem.at[number[name]],
            device_id=devices[queue],
            device_id_type=MESH,
        )

    def make_tables():
        own[2].wait()
        own[3].wait()
        shape = (N_LAYER, PHASE)
        fields = [
            jnp.concatenate([plan_v[s, f] for s in range(LISTS)], axis=1) for f in range(3)
        ]
        limit = jnp.concatenate(
            [jnp.broadcast_to(counts_v[:, s : s + 1], (N_LAYER, PCAP)) for s in range(LISTS)], axis=1
        )
        left, right, target = fields
        at = lax.broadcasted_iota(jnp.int32, shape, 1)
        s = at // PCAP
        column = (left // (N_LAYER * ACAP) + N_COL - c) % N_COL
        x_on = (s // 2 + N_X - r // 2) % N_X
        core_on = (s + r) % 2
        live = at % PCAP < limit
        key = jnp.where(live, target, CL) * PHASE + at
        packed = (target * PHASE + column * ACAP + left % ACAP) * PHASE
        packed = packed + (x_on * 2 + core_on) * BCAP + right
        rank = jnp.zeros(shape, jnp.int32)
        for q in range(PHASE):
            rank += jnp.where(jnp.broadcast_to(key[:, q : q + 1], shape) < key, 1, 0)
        ordered, place, last = packed, target, jnp.full(shape, -1, jnp.int32)
        sort_key = key // PHASE
        for q in range(PHASE):
            here = at == jnp.broadcast_to(rank[:, q : q + 1], shape)
            ordered = jnp.where(here, jnp.broadcast_to(packed[:, q : q + 1], shape), ordered)
            place = jnp.where(here, jnp.broadcast_to(sort_key[:, q : q + 1], shape), place)
            one = jnp.broadcast_to(sort_key[:, q : q + 1], shape)
            last = jnp.where(at == one, jnp.maximum(last, jnp.broadcast_to(rank[:, q : q + 1], shape)), last)
        earlier = jnp.concatenate([place[:, 0:1] - 1, place[:, 0 : PHASE - 1]], axis=1)
        table_v[0:4] = ordered // PHASE % PHASE
        table_v[4:8] = ordered % PHASE
        table_v[8:12] = ordered // (PHASE * PHASE)
        table_v[12:16] = jnp.where(place == earlier, 0, 1)
        table_v[16:20] = jnp.where(last < 0, PHASE + at, last)

    def wait_for(sem, blocks):
        window = chain.at[pl.ds(0, blocks)]
        pltpu.make_async_copy(window, window, sem).wait()

    def split(slot, blocks):
        if slot[0] == "A":
            base, halves, land = slot[2] * ACAP, a_half, a_land
        else:
            base, halves, land = (slot[2] * 2 + slot[3]) * BCAP, b_half, b_land

        def one(block):
            value = land[(*slot[1:], block)]
            high = value.astype(jnp.bfloat16)
            low = (value - high.astype(jnp.float32)).astype(jnp.bfloat16)
            halves[slot[1], base + block, :, 0:BS] = high
            halves[slot[1], base + block, :, BS : 2 * BS] = low

        def two(step, carry):
            one(blocks[0] + 2 * step)
            one(blocks[0] + 2 * step + 1)
            return carry

        pairs, odd = divmod(blocks[1] - blocks[0], 2)
        lax.fori_loop(0, pairs, two, 0)
        if odd:
            one(blocks[1] - 1)

    def multiply(d, total):
        m = lax.rem(o + d, N_LAYER)
        unroll = UNROLL[d]

        def some(index, total):
            for p in range(unroll):
                at = index * unroll + p
                left = a_half[d, table_s[m, at]]
                right = b_half[d, table_s[4 + m, at]]
                both = jnp.dot(
                    left,
                    jnp.concatenate([right, right], axis=0),
                    preferred_element_type=jnp.float32,
                )
                first = jnp.broadcast_to(table_s[12 + m, at], (BS, BS)) == 1
                total = jnp.where(first, sums[table_s[8 + m, at]], total)
                total = total + (both[:, 0:BS] + both[:, BS : 2 * BS])
                chain[at] = total
            return total

        return lax.fori_loop(0, PHASE // unroll, some, total)

    def collect(d):
        m = lax.rem(o + d, N_LAYER)

        def some(step, carry):
            for k in range(4):
                t = step * 4 + k
                total = chain[table_s[16 + m, t]]
                if d == ORDER[-1]:
                    out_ref[t] = total
                else:
                    sums[t] = total
                    chain[PHASE + t] = total
            return carry

        lax.fori_loop(0, CL // 4, some, 0)

    def clear(t, carry):
        sums[t] = jnp.zeros((BS, BS), jnp.float32)
        chain[PHASE + t] = jnp.zeros((BS, BS), jnp.float32)
        return carry

    scalars, running = "none", jnp.zeros((BS, BS), jnp.float32)
    for step in steps:
        if step[0] == "send":
            copies[step[1]].start()
        elif step[0] == "tables":
            make_tables()
            lax.fori_loop(0, CL, clear, 0)
        elif step[0] == "wait":
            names = together[step[1]]
            if len(names) == 1:
                copies[names[0]].wait_recv()
            else:
                wait_for(recv_sem.at[number[names[0]]], size[number[names[0]]])
            if scalars == "none":
                to_scalar.start()
                scalars = "started"
        elif step[0] == "split":
            split(*step[1:])
        else:
            if scalars == "started":
                to_scalar.wait()
                scalars = "there"
            running = multiply(step[1], running)
            collect(step[1])
    for pool in range(2):
        wait_for(send_sem.at[pool], sent[pool])


def per_device(a_blocks, b_blocks, pair_plan, pair_counts):
    count = len(groups())
    hbm = pl.BlockSpec(memory_space=pltpu.HBM)
    plan = pair_plan[0, 0, 0].transpose(0, 2, 1, 3)
    operands = (a_blocks[0], b_blocks[:, 0], plan, pair_counts[0, 0, 0].T)
    result = pl.pallas_call(
        kernel,
        out_shape=jax.ShapeDtypeStruct((CL, BS, BS), jnp.float32),
        in_specs=[hbm, hbm, hbm, hbm],
        out_specs=pl.BlockSpec(memory_space=pltpu.VMEM),
        scratch_shapes=[
            pltpu.VMEM((N_LAYER, N_COL, ACAP, BS, BS), jnp.float32),
            pltpu.VMEM((N_LAYER, N_X, 2, BCAP, BS, BS), jnp.float32),
            pltpu.VMEM((N_LAYER, N_COL * ACAP, BS, 2 * BS), jnp.bfloat16),
            pltpu.VMEM((N_LAYER, N_ROW * BCAP, BS, 2 * BS), jnp.bfloat16),
            pltpu.VMEM((PHASE + CL, BS, BS), jnp.float32),
            pltpu.VMEM((CL, BS, BS), jnp.float32),
            pltpu.VMEM((N_ROW, 3, N_LAYER, PCAP), jnp.int32),
            pltpu.VMEM((N_LAYER, N_ROW), jnp.int32),
            pltpu.VMEM((24, PHASE), jnp.int32),
            pltpu.SMEM((24, PHASE), jnp.int32),
            pltpu.SemaphoreType.DMA((5,)),
            pltpu.SemaphoreType.DMA((2,)),
            pltpu.SemaphoreType.DMA((count,)),
        ],
        compiler_params=pltpu.CompilerParams(
            collective_id=0, has_side_effects=True, vmem_limit_bytes=50 * 1024 * 1024
        ),
        name="gather_multiply",
    )(*[pltpu.with_memory_space_constraint(x, pltpu.HBM) for x in operands])
    return result[None, None]


def solution(mesh):
    in_specs = (
        P("row", ("col", "layer"), None, None),
        P(("row", "layer"), "col", None, None),
        P("row", "col", "layer", None, None, None, None),
        P("row", "col", "layer", None, None),
    )
    out_specs = P("row", "col", "layer", None, None)
    return jax.shard_map(
        per_device, mesh=mesh, in_specs=in_specs, out_specs=out_specs, check_vma=False
    )
```
